32 devices in a mesh: dom: 32 (over z, y, x, core).
Axes of the slice: x: 2, y: 2, z: 4, core: 2. Of those that a mesh axis runs over, the one named last changes fastest.
Arguments:
- features: bfloat16 [16384, 512], P('dom'), may hold values from -6 to 6
- weights: bfloat16 [3, 512, 512], replicated, may hold values from -0.078125 to 0.078125
- halo_send: int32 [32, 32, 4], P('dom'), may hold values from 0 to 511
- nbr_index: int32 [16384, 2, 8], P('dom'), may hold values from 0 to 639
- tile_count: int32 [32], P('dom'), may hold values from 1 to 16, as said below
- edge_ends: int32 [512, 2, 256], P('dom'), may hold values from 0 to 511
- neg_ids: int32 [256], P('dom'), may hold values from 0 to 511
Outputs:
- weight_grad: float32 [3, 512, 512], replicated
- mean_loss: float32 [], replicated
- pre_grad: bfloat16 [16384, 512], P('dom')
The draws below stay inside these ranges and needn't reach their ends.
Inputs may be any that keep to these rules, and one draw needn't show every extreme that they name: `nbr_index`: an entry below 512 names a row of the node's own partition; an entry 512 + q * 4 + k names slot k of the halo from partition q. `tile_count`: partition 32 - 1 holds 16 tiles; every other partition holds at most 8. `edge_ends`: tile slots at or past a partition's tile_count hold no edges. `neg_ids`: entry j names a row of partition j // 8.
All inputs are finite; a program needn't handle non-finite values.
Results may differ from the reference program's by a relative error of at most 0.0012.
The reference program's roundings to bfloat16 on the way count: a program that leaves them out, or rounds other values in their place, can miss the bound.
Values may be sent and summed in bfloat16 or wider, within the bound.
A program may use at most 64 MiB of HBM per device.

```python
import jax
import jax.numpy as jnp
from jax import lax

H = 512
RELS = 2
FAN = 8
TILE = 256
NODE_DEV = 512
HALO_PEER = 4
MAX_TILES = 16
NEG_DEV = 8
NODES = 16384
NEG = 256
SLOTS = 640
N_DOM = 32


def draw_tile_count(key, part):
    first = jax.random.randint(jax.random.fold_in(key, 11), (N_DOM,), 0, MAX_TILES)
    second = jax.random.randint(jax.random.fold_in(key, 12), (N_DOM,), 0, MAX_TILES)
    counts = 1 + first * second // (2 * MAX_TILES)
    return jnp.where(jnp.arange(N_DOM) == N_DOM - 1, MAX_TILES, counts).astype(jnp.int32)


def touch_ends(values, own_key, low, top_value):
    longest = values.shape.index(max(values.shape))
    spots = []
    for shift in (0, 1):
        where = [jax.random.randint(jax.random.fold_in(own_key, axis), (), 0, length) for axis, length in enumerate(values.shape)]
        where[longest] = (where[longest] + shift) % values.shape[longest]
        spots.append(tuple(where))
    return values.at[spots[0]].set(low).at[spots[1]].set(top_value)


def levels(key, dims, split, low, largest):
    def one(axis_at, blocks):
        steps = jax.random.uniform(jax.random.fold_in(jax.random.fold_in(key, 6), axis_at), (blocks,), jnp.float32, low / len(split), largest / len(split))
        return jnp.repeat(jnp.exp(steps), dims[axis_at] // blocks).reshape((-1,) + (1,) * (len(dims) - axis_at - 1))

    factor_of = one(*split[0])
    for cut in split[1:]:
        factor_of = factor_of * one(*cut)
    return factor_of


def centred(key, extent, scale, limit, split=(), kind=jnp.bfloat16):
    entries = jax.random.normal(key, extent, jnp.float32) * scale
    if len(split) > 0:
        entries = levels(key, extent, split, -0.22, 0.18) * entries
    return jnp.clip(entries, min=-limit, max=limit).astype(kind)


def setup_inputs(seed: int = 0) -> dict:
    seeds = jax.random.split(jax.random.key(seed), 8)
    return {
        "features": centred(seeds[0], (NODES, H), 1.0, 6.0, ((0, 32),)),
        "weights": centred(seeds[1], (RELS + 1, H, H), (12 * H) ** -0.5, 0.078125),
        "halo_send": touch_ends(jax.random.randint(seeds[2], (N_DOM, N_DOM, HALO_PEER), 0, NODE_DEV), jax.random.fold_in(seeds[2], 1), 0, NODE_DEV - 1).astype(jnp.int32),
        "nbr_index": touch_ends(jax.random.randint(seeds[3], (NODES, RELS, FAN), 0, SLOTS), jax.random.fold_in(seeds[3], 1), 0, SLOTS - 1).astype(jnp.int32),
        "tile_count": draw_tile_count(jax.random.fold_in(seeds[7], 71), 0),
        "edge_ends": touch_ends(jax.random.randint(seeds[5], (N_DOM * MAX_TILES, 2, TILE), 0, NODE_DEV), jax.random.fold_in(seeds[5], 1), 0, NODE_DEV - 1).astype(jnp.int32),
        "neg_ids": touch_ends(jax.random.randint(seeds[6], (NEG,), 0, NODE_DEV), jax.random.fold_in(seeds[6], 1), 0, NODE_DEV - 1).astype(jnp.int32),
    }


def neighbour_mean(lookup, neighbours):
    running_sum = jnp.zeros((neighbours.shape[0], lookup.shape[1]), jnp.float32)
    for column in range(neighbours.shape[1]):
        running_sum = running_sum + lookup[neighbours[:, column]].astype(jnp.float32)
    return (running_sum / neighbours.shape[1]).astype(jnp.bfloat16)


def score_tile(source, target, negatives):
    source_wide = source.astype(jnp.float32)
    target_wide = target.astype(jnp.float32)
    positive = jnp.sum(source_wide * target_wide, axis=1)
    negative = lax.dot_general(source, negatives, (((1,), (1,)), ((), ())), preferred_element_type=jnp.float32)
    count_neg = negatives.shape[0]
    tile_loss = jnp.sum(jnp.logaddexp(0.0, -positive)) + jnp.sum(jnp.logaddexp(0.0, negative)) / count_neg
    grad_positive = -jax.nn.sigmoid(-positive)
    grad_negative = (jax.nn.sigmoid(negative) / count_neg).astype(jnp.bfloat16)
    source_grad = grad_positive[:, None] * target_wide + jnp.dot(grad_negative, negatives, preferred_element_type=jnp.float32)
    target_grad = grad_positive[:, None] * source_wide
    negative_grad = lax.dot_general(grad_negative, source, (((0,), (0,)), ((), ())), preferred_element_type=jnp.float32)
    return tile_loss, source_grad, target_grad, negative_grad


def reference(features, weights, halo_send, nbr_index, tile_count, edge_ends, neg_ids):
    def layer_part(partition):
        own_rows = lax.dynamic_slice_in_dim(features, partition * NODE_DEV, NODE_DEV, 0)
        sender = jnp.arange(N_DOM, dtype=jnp.int32)[:, None] * NODE_DEV
        halo_index = (sender + halo_send[:, partition, :]).reshape(-1).astype(jnp.int32)
        lookup = jnp.concatenate([own_rows, features[halo_index]], 0)
        neighbours = lax.dynamic_slice_in_dim(nbr_index, partition * NODE_DEV, NODE_DEV, 0)
        preact = jnp.dot(own_rows, weights[0], preferred_element_type=jnp.float32)
        means = []
        for relation in range(RELS):
            mean_rows = neighbour_mean(lookup, neighbours[:, relation, :])
            means.append(mean_rows)
            preact = preact + jnp.dot(mean_rows, weights[relation + 1], preferred_element_type=jnp.float32)
        return preact, jnp.stack(means)

    parts = jnp.arange(N_DOM, dtype=jnp.int32)
    preact, means = lax.map(layer_part, parts)
    embedding = preact.astype(jnp.bfloat16)
    flat_rows = embedding.reshape(-1, H)
    neg_rows = (jnp.arange(NEG, dtype=jnp.int32) // NEG_DEV) * NODE_DEV + neg_ids
    negatives = flat_rows[neg_rows]

    def per_part(state_now, partition):
        loss_sum, negative_total = state_now
        own_embed = embedding[partition]
        tile_ends = lax.dynamic_slice_in_dim(edge_ends, partition * MAX_TILES, MAX_TILES, 0)

        def tile_step(tile_index, running):
            tile_loss_sum, node_grad, neg_grad = running
            pair_ends = lax.dynamic_index_in_dim(tile_ends, tile_index, 0, keepdims=False)
            tile_loss, source_grad, target_grad, negative_grad = score_tile(own_embed[pair_ends[0]], own_embed[pair_ends[1]], negatives)
            node_grad = node_grad.at[pair_ends[0]].add(source_grad).at[pair_ends[1]].add(target_grad)
            return tile_loss_sum + tile_loss, node_grad, neg_grad + negative_grad

        initial = (jnp.zeros((), jnp.float32), jnp.zeros((NODE_DEV, H), jnp.float32), negative_total)
        tile_loss_sum, node_grad, negative_total = lax.fori_loop(0, tile_count[partition], tile_step, initial)
        return (loss_sum + tile_loss_sum, negative_total), node_grad

    start_state = (jnp.zeros((), jnp.float32), jnp.zeros((NEG, H), jnp.float32))
    (loss_sum, negative_total), node_grad = lax.scan(per_part, start_state, parts)
    node_grad = node_grad.reshape(-1, H).at[neg_rows].add(negative_total).reshape(N_DOM, NODE_DEV, H)
    pre_grad = node_grad.astype(jnp.bfloat16)
    feature_parts = features.reshape(N_DOM, NODE_DEV, H)

    def grad_part(running, items):
        own_rows, mean_rows, grad_rows = items
        terms = [lax.dot_general(own_rows, grad_rows, (((0,), (0,)), ((), ())), preferred_element_type=jnp.float32)]
        for relation in range(RELS):
            terms.append(lax.dot_general(mean_rows[relation], grad_rows, (((0,), (0,)), ((), ())), preferred_element_type=jnp.float32))
        return running + jnp.stack(terms), None

    weight_sum, unused = lax.scan(grad_part, jnp.zeros((RELS + 1, H, H), jnp.float32), (feature_parts, means, pre_grad))
    edge_total = jnp.sum(tile_count).astype(jnp.float32) * TILE
    return weight_sum / edge_total, loss_sum / edge_total, pre_grad.reshape(-1, H)
```

```python
import functools
import itertools

import jax
import jax.numpy as jnp
from jax import lax
from jax.experimental import pallas as pl
from jax.experimental.pallas import tpu as pltpu
from jax.sharding import PartitionSpec as P

F32 = jnp.float32
BF16 = jnp.bfloat16
VMEM_LIMIT = 48 * 1024 * 1024
LANES = 128
STEPS = 32700.0
TINY = 1e-30
MESH = pl.DeviceIdType.MESH


def whole(count):
    return [pl.BlockSpec(memory_space=pltpu.VMEM)] * count


def nn(a, b):
    return jnp.dot(a, b, preferred_element_type=F32)


def nt(a, b):
    return lax.dot_general(a, b, (((1,), (1,)), ((), ())), preferred_element_type=F32)


def tn(a, b):
    return lax.dot_general(a, b, (((0,), (0,)), ((), ())), preferred_element_type=F32)


def halves(x):
    high = x.astype(BF16)
    return high, (x - high.astype(F32)).astype(BF16)


def one_hot(mask):
    return jnp.where(mask, 1.0, 0.0).astype(BF16)


def prepare_kernel(fan, nbr_ref, ends_ref, count_ref, table_ref, pairs_ref, degree_ref):
    nodes, slots = table_ref.shape[1:]
    step = 64

    @pl.loop(0, nodes // step)
    def _(block):
        rows = pl.ds(pl.multiple_of(block * step, step), step)
        lanes = lax.broadcasted_iota(jnp.int32, (step, slots), 1)
        named = nbr_ref[rows, :]
        for relation in range(table_ref.shape[0]):
            total = jnp.zeros((step, slots), F32)
            for k in range(fan):
                column = relation * fan + k
                total = total + jnp.where(named[:, column : column + 1] == lanes, 1.0, 0.0)
            table_ref[relation, rows, :] = total.astype(BF16)

    pairs_ref[...] = jnp.zeros_like(pairs_ref)

    @pl.loop(0, count_ref[0])
    def _(tile):
        ends = ends_ref[tile]
        rows = lax.broadcasted_iota(jnp.int32, (nodes, ends.shape[1]), 0)
        pairs_ref[...] += nt(one_hot(ends[0:1, :] == rows), one_hot(ends[1:2, :] == rows))

    pairs = pairs_ref[...]
    degree_ref[...] = jnp.sum(pairs, axis=1, keepdims=True)
    pairs_ref[...] = pairs + pairs.T


def layer_kernel(fan, own_ref, halo_ref, weights_ref, table_ref, ids_ref, means_ref, embed_ref, neg_ref, left_ref):
    nodes = own_ref.shape[0]
    own = own_ref[...]
    preact = nn(own, weights_ref[0])
    for relation in range(table_ref.shape[0]):
        total = nn(table_ref[relation, :, :nodes], own) + nn(table_ref[relation, :, nodes:], halo_ref[...])
        mean = (total / fan).astype(BF16)
        means_ref[relation] = mean
        preact = preact + nn(mean, weights_ref[relation + 1])
    embedding = preact.astype(BF16)
    embed_ref[...] = embedding
    lanes = lax.broadcasted_iota(jnp.int32, (ids_ref.shape[0], nodes), 1)
    slot, ids = id_column(ids_ref)
    neg_ref[...] = nn(one_hot(ids == lanes), embedding).astype(BF16)
    again = jnp.zeros_like(ids)
    for j in range(ids_ref.shape[0]):
        again = again + jnp.where((ids == ids_ref[j]) & (slot > j), 1, 0)
    pick = one_hot((ids == lanes) & (again == 0))
    left_ref[0] = nn(pick, own).astype(BF16)
    for relation in range(table_ref.shape[0]):
        left_ref[relation + 1] = nn(pick, means_ref[relation]).astype(BF16)


def score_kernel(
    parts, embed_ref, pairs_ref, degree_ref, mine_ref, left_ref, count_ref, edge_ref,
    grad_ref, pre_ref, neg_ref, stats_ref, lefts_ref, landed, positive, send_sem, recv_sem, left_send, left_recv
):
    me = lax.axis_index("dom")
    barrier = pltpu.get_barrier_semaphore()

    def copy_to(peer, slot, sem):
        return pltpu.make_async_remote_copy(
            src_ref=mine_ref,
            dst_ref=landed.at[slot],
            send_sem=send_sem.at[sem],
            recv_sem=recv_sem.at[slot],
            device_id=(peer,),
            device_id_type=MESH,
        )

    @pl.loop(1, parts)
    def _(i):
        pl.semaphore_signal(barrier, inc=1, device_id=((me + i) % parts,), device_id_type=MESH)

    pl.semaphore_wait(barrier, parts - 1)

    @pl.loop(1, parts)
    def _(i):
        copy_to((me + i) % parts, me, i).start()

    core, place, chips = me % 2, me // 2, parts // 2

    def left_to(other, slot, sem):
        return pltpu.make_async_remote_copy(
            src_ref=left_ref,
            dst_ref=lefts_ref.at[slot],
            send_sem=left_send.at[sem],
            recv_sem=left_recv.at[slot],
            device_id=(2 * other + core,),
            device_id_type=MESH,
        )

    @pl.loop(1, chips)
    def _(i):
        left_to((place + i) % chips, place, i).start()

    lefts_ref[place] = left_ref[...]
    landed[me] = mine_ref[...]
    embedding = embed_ref[...]
    pairs = pairs_ref[...]
    score = nt(embedding, embedding)
    small = jnp.exp(-jnp.abs(score))
    positive_loss = 0.5 * jnp.sum(pairs * (jnp.maximum(-score, 0.0) + jnp.log1p(small)))
    high, low = halves(-pairs * (jnp.where(score >= 0, small, 1.0) / (1.0 + small)))
    positive[...] = nn(high, embedding) + nn(low, embedding)

    @pl.loop(1, parts)
    def _(i):
        copy_to((me + i) % parts, (me + i) % parts, i).wait()

    own_neg, width = mine_ref.shape
    negatives = landed[...].reshape(parts * own_neg, width)
    degree = degree_ref[...]
    count = negatives.shape[0]
    score = nt(embedding, negatives)
    small = jnp.exp(-jnp.abs(score))
    loss = jnp.maximum(score, 0.0) + jnp.log1p(small)
    loss_sum = positive_loss + jnp.sum(degree * loss) / count
    slope = ((jnp.where(score >= 0, 1.0, small) / (1.0 + small)) / count).astype(BF16)
    grad = positive[...] + degree * nn(slope, negatives)
    grad_ref[...] = grad
    pre_ref[...] = grad.astype(BF16)
    high, low = halves(degree * embedding.astype(F32))
    neg_ref[...] = tn(slope, high) + tn(slope, low)
    edges = count_ref[0].astype(F32) * edge_ref.shape[1]
    rows = lax.broadcasted_iota(jnp.int32, stats_ref.shape, 0)
    stats_ref[...] = jnp.where(rows == 2, loss_sum, edges)

    @pl.loop(1, chips)
    def _(i):
        left_to((place + i) % chips, (place + i) % chips, i).wait()


def greet(peers):
    barrier = pltpu.get_barrier_semaphore()
    for peer in peers:
        pl.semaphore_signal(barrier, inc=1, device_id=(peer,), device_id_type=MESH)
    pl.semaphore_wait(barrier, len(peers))


def greet(peers):
    barrier = pltpu.get_barrier_semaphore()
    for peer in peers:
        pl.semaphore_signal(barrier, inc=1, device_id=(peer,), device_id_type=MESH)
    pl.semaphore_wait(barrier, len(peers))


def layout(parts):
    radix = [1, 1, 1]
    at = 0
    while radix[0] * radix[1] * radix[2] * 2 < parts:
        radix[at % 3] *= 2
        at += 1
    outer, middle, inner = radix
    first, second, last = (inner, 2), (middle, 2 * inner), (outer, 2 * inner * middle)
    return [[first, second, last], [second, first, last]]


def sizes(axes):
    return tuple(size for size, _ in axes)


def device_of(axes, core, spot):
    return core + sum(at * stride for at, (_, stride) in zip(spot, axes))


def spots_of(axes):
    return itertools.product(*(range(size) for size, _ in axes))


def id_column(ids_ref):
    count = ids_ref.shape[0]
    rows = lax.broadcasted_iota(jnp.int32, (count, 1), 0)
    column = jnp.zeros((count, 1), jnp.int32)
    for j in range(count):
        column = jnp.where(rows == j, ids_ref[j], column)
    return rows, column


def quantize(x, scale):
    return jnp.round(x * (1.0 / scale)).astype(jnp.int32).astype(jnp.int16)


def lane_scale(x):
    top = jnp.max(jnp.abs(x).reshape(-1, x.shape[-1]), axis=0, keepdims=True)
    return jnp.maximum(top, TINY) * (1.0 / STEPS)


def reduce_kernel(colors, own_ref, means_ref, grad_ref, neg_ref, lefts_ref, stats_ref, ids_ref, *refs):
    count = len(colors)
    terms = means_ref.shape[0] + 1
    me = lax.axis_index("dom")
    core = me % 2
    partner = me + 1 - 2 * core
    refs = list(refs)

    def take(number):
        taken = refs[:number]
        del refs[:number]
        return taken

    words, scales, rows_out = take(count), take(count), take(count)
    lefts_out, total_ref = take(2)
    full, full_neg, paired, paired_neg = take(count), take(count), take(count), take(count)
    sums, sums_neg = [take(3) for _ in colors], [take(3) for _ in colors]
    out_q, out_n, out_m = [take(3) for _ in colors], [take(3) for _ in colors], [take(3) for _ in colors]
    in_q, in_n, in_m = [take(3) for _ in colors], [take(3) for _ in colors], [take(3) for _ in colors]
    stats_in, send_sem, recv_sem = take(3)
    spots = {}

    def remote(source, target, key, peer):
        at = spots.setdefault(key, len(spots))
        return pltpu.make_async_remote_copy(
            src_ref=source,
            dst_ref=target,
            send_sem=send_sem.at[at],
            recv_sem=recv_sem.at[at],
            device_id=(peer,),
            device_id_type=MESH,
        )

    def mine(axis):
        size, stride = axis
        return (me // stride) % size

    peers = [partner]
    for size, stride in colors[0]:
        at = (me // stride) % size
        peers += [me + ((at + delta) % size - at) * stride for delta in range(1, size)]
    greet(peers)
    lefts_copy = remote(lefts_ref, lefts_out.at[core], "lefts", partner)
    lefts_copy.start()
    stats_copy = remote(stats_ref, stats_in, "stats", partner)
    stats_copy.start()

    nodes, width = grad_ref.shape
    own_neg = ids_ref.shape[0]
    slot, ids = id_column(ids_ref)
    node = lax.broadcasted_iota(jnp.int32, (nodes, 1), 0)
    named = jnp.zeros((nodes, 1), jnp.bool_)
    for j in range(own_neg):
        named = named | (node == ids_ref[j])
    pre = jnp.where(named, 0.0, grad_ref[...]).astype(BF16)
    lanes = lax.broadcasted_iota(jnp.int32, (own_neg, nodes), 1)
    pick = jnp.where(ids == lanes, 1.0, 0.0)
    local = jnp.dot(pick, grad_ref[...], preferred_element_type=F32, precision=lax.Precision.HIGHEST)
    rows = full[0].shape[5]
    pairs = []
    wide = 2 * LANES
    for half in range(0, count, 2):
        lanes = slice(half * LANES, half * LANES + wide)
        for color in (half, half + 1):
            axes = colors[color]
            for c in range(2):
                for spot in spots_of(axes):
                    at = device_of(axes, c, spot) * own_neg
                    full_neg[color][(c, *spot)] = neg_ref[at : at + own_neg, color * LANES : (color + 1) * LANES]
        for term in range(terms):
            left = own_ref[...] if term == 0 else means_ref[term - 1]
            product = tn(left, pre[:, lanes])
            for color in (half, half + 1):
                axes = colors[color]
                part = product[:, (color - half) * LANES : (color - half + 1) * LANES]
                for c in range(2):
                    for spot in spots_of(axes):
                        at = device_of(axes, c, spot) * rows
                        full[color][(c, *spot, term)] = part[at : at + rows]
        for color in (half, half + 1):
            pairs.append([
                remote(full[color].at[1 - core], paired[color], ("pair", color), partner),
                remote(full_neg[color].at[1 - core], paired_neg[color], ("pair_neg", color), partner),
            ])
            for copy in pairs[-1]:
                copy.start()

    def scatter(color, phase, stats):
        axis = colors[color][phase]
        size, stride = axis
        at = mine(axis)
        copies = []
        for delta in range(1, size):
            other = (at + delta) % size
            peer = me + (other - at) * stride
            block, neg = sums[color][phase][other], sums_neg[color][phase][other]
            scale, neg_scale = lane_scale(block), lane_scale(neg)
            spot = delta - 1
            out_q[color][phase][spot] = quantize(block, scale)
            out_n[color][phase][spot] = quantize(neg, neg_scale)
            out_m[color][phase][spot, 0:1] = scale
            out_m[color][phase][spot, 1:2] = neg_scale
            out_m[color][phase][spot, 2:4] = stats
            key = ("scatter", color, phase, delta)
            copies += [
                remote(out_q[color][phase].at[spot], in_q[color][phase].at[spot], (*key, 0), peer),
                remote(out_n[color][phase].at[spot], in_n[color][phase].at[spot], (*key, 1), peer),
                remote(out_m[color][phase].at[spot], in_m[color][phase].at[at], (*key, 2), peer),
            ]
        for copy in copies:
            copy.start()
        return copies

    def gather(color, phase):
        axes = colors[color]
        at = [mine(axis) for axis in axes]
        index = (core, *at[: phase + 1])
        copies = []
        if phase < 0:
            for kind, ref in enumerate((words[color], scales[color], rows_out[color])):
                copies.append(remote(ref.at[core], ref.at[core], ("gather", color, phase, 0, kind), partner))
        else:
            size, stride = axes[phase]
            for delta in range(1, size):
                peer = me + ((at[phase] + delta) % size - at[phase]) * stride
                for kind, ref in enumerate((words[color], scales[color], rows_out[color])):
                    copies.append(remote(ref.at[index], ref.at[index], ("gather", color, phase, delta, kind), peer))
        for copy in copies:
            copy.start()
        return copies

    lefts_out[core] = lefts_ref[...]
    stats_copy.wait()
    stats = [None] * count
    stats[0] = stats_ref[2:4] + stats_in[2:4]
    for color in range(1, count):
        stats[color] = stats[0]
    flying = []
    for color in range(count):
        for copy in pairs[color]:
            copy.wait()
        sums[color][0][...] = full[color][core] + paired[color][...]
        sums_neg[color][0][...] = full_neg[color][core] + paired_neg[color][...]
        flying.append(scatter(color, 0, stats[color]))
    for phase in range(3):
        for color in range(count):
            axis = colors[color][phase]
            size = axis[0]
            at = mine(axis)
            for copy in flying[color]:
                copy.wait()
            total = sums[color][phase][at]
            total_neg = sums_neg[color][phase][at]
            for delta in range(1, size):
                meta = in_m[color][phase][(at + size - delta) % size]
                total = total + in_q[color][phase][delta - 1].astype(jnp.int32).astype(F32) * meta[0:1]
                total_neg = total_neg + in_n[color][phase][delta - 1].astype(jnp.int32).astype(F32) * meta[1:2]
            in_m[color][phase][at, 2:4] = stats[color]
            stats[color] = in_m[color][phase][0, 2:4]
            for position in range(1, size):
                stats[color] = stats[color] + in_m[color][phase][position, 2:4]
            if phase < 2:
                sums[color][phase + 1][...] = total
                sums_neg[color][phase + 1][...] = total_neg
                flying[color] = scatter(color, phase + 1, stats[color])
            else:
                index = (core, *(mine(a) for a in colors[color]))
                scale = lane_scale(total)
                words[color][index] = quantize(total, scale)
                scales[color][index] = scale
                gathered = local[:, color * LANES : (color + 1) * LANES]
                for j in range(own_neg):
                    gathered = gathered + jnp.where(ids == ids_ref[j], total_neg[j : j + 1], 0.0)
                rows_out[color][index] = gathered.astype(BF16)
                flying[color] = gather(color, 2)
    total_ref[0:2] = stats[0]
    for phase in (1, 0, -1):
        for color in range(count):
            for copy in flying[color]:
                copy.wait()
            flying[color] = gather(color, phase)
    for color in range(count):
        for copy in flying[color]:
            copy.wait()
    lefts_copy.wait()


def finish_kernel(colors, ids_ref, pre_ref, lefts_ref, total_ref, *refs):
    count = len(colors)
    words, scales, rows_in = refs[:count], refs[count : 2 * count], refs[2 * count : 3 * count]
    out_ref, loss_ref, pre_out, joint = refs[3 * count :]
    term = pl.program_id(0)
    own_neg = ids_ref.shape[0]
    chips = lefts_ref.shape[1]
    edges = total_ref[1:2]
    inverse = 1.0 / edges

    @pl.when(term == 0)
    def _():
        me = lax.axis_index("dom")
        loss_ref[...] = total_ref[0:1] / edges
        for color, axes in enumerate(colors):
            for c in range(2):
                for spot in spots_of(axes):
                    at = (c * chips + device_of(axes, 0, spot) // 2) * own_neg
                    joint[at : at + own_neg, color * LANES : (color + 1) * LANES] = rows_in[color][(c, *spot)]
        slot, ids = id_column(ids_ref)
        again = jnp.zeros_like(ids)
        for j in range(own_neg):
            again = again + jnp.where((ids == ids_ref[j]) & (slot > j), 1, 0)
        nodes = pre_ref.shape[0]
        lanes = lax.broadcasted_iota(jnp.int32, (own_neg, nodes), 1)
        pick = one_hot((ids == lanes) & (again == 0))
        node = lax.broadcasted_iota(jnp.int32, (nodes, 1), 0)
        named = jnp.zeros((nodes, 1), jnp.bool_)
        for j in range(own_neg):
            named = named | (node == ids_ref[j])
        for color, axes in enumerate(colors):
            block = slice(color * LANES, (color + 1) * LANES)
            index = (me % 2, *((me // stride) % size for size, stride in axes))
            patch = tn(pick, rows_in[color][index])
            pre_out[:, block] = jnp.where(named, patch, pre_ref[:, block].astype(F32)).astype(BF16)

    lefts = lefts_ref[:, :, term].reshape(2 * chips * own_neg, lefts_ref.shape[4])
    extra = tn(lefts, joint[...])
    rows = words[0].shape[5]
    for color, axes in enumerate(colors):
        block = slice(color * LANES, (color + 1) * LANES)
        for c in range(2):
            for spot in spots_of(axes):
                at = device_of(axes, c, spot) * rows
                value = words[color][(c, *spot, term)].astype(jnp.int32).astype(F32) * scales[color][(c, *spot)]
                out_ref[0, at : at + rows, block] = (value + extra[at : at + rows, block]) * inverse


def call(kernel, out_shape, in_specs, collective=None, **kwargs):
    extra = {} if collective is None else {"collective_id": collective, "has_side_effects": True}
    many = isinstance(out_shape, (list, tuple))
    return pl.pallas_call(
        kernel,
        out_shape=out_shape,
        in_specs=in_specs,
        out_specs=whole(len(out_shape)) if many else whole(1)[0],
        compiler_params=pltpu.CompilerParams(vmem_limit_bytes=VMEM_LIMIT, **extra),
        **kwargs,
    )


def shape(dims, kind):
    return jax.ShapeDtypeStruct(dims, kind)


def on_device(parts, features, weights, halo_send, nbr_index, tile_count, edge_ends, neg_ids):
    nodes, width = features.shape
    relations, fan = nbr_index.shape[1:]
    per_peer = halo_send.shape[2]
    slots = nodes + parts * per_peer
    own_neg = neg_ids.shape[0]
    wanted = halo_send.reshape(-1, 1)
    columns = lax.broadcasted_iota(jnp.int32, (parts * per_peer, nodes), 1)
    outgoing = nn((wanted == columns).astype(BF16), features).astype(BF16)
    incoming = lax.all_to_all(
        outgoing.reshape(parts, per_peer, width), "dom", split_axis=0, concat_axis=0, tiled=True
    ).reshape(-1, width)
    table, pairs, degree = call(
        functools.partial(prepare_kernel, fan),
        (
            shape((relations, nodes, slots), BF16),
            shape((nodes, nodes), F32),
            shape((nodes, 1), F32),
        ),
        whole(2) + [pl.BlockSpec(memory_space=pltpu.SMEM)],
    )(nbr_index.reshape(nodes, relations * fan), edge_ends, tile_count)
    smem = pl.BlockSpec(memory_space=pltpu.SMEM)
    chips = parts // 2
    means, embedding, my_negs, my_lefts = call(
        functools.partial(layer_kernel, fan),
        (
            shape((relations, nodes, width), BF16),
            shape((nodes, width), BF16),
            shape((own_neg, width), BF16),
            shape((relations + 1, own_neg, width), BF16),
        ),
        whole(4) + [smem],
    )(features, incoming, weights, table, neg_ids)
    node_grad, pre, neg_grad, stats, lefts = call(
        functools.partial(score_kernel, parts),
        (
            shape((nodes, width), F32),
            shape((nodes, width), BF16),
            shape((parts * own_neg, width), F32),
            shape((8, LANES), F32),
            shape((chips, relations + 1, own_neg, width), BF16),
        ),
        whole(5) + [smem, pl.BlockSpec(memory_space=pltpu.VMEM)],
        collective=3,
        scratch_shapes=[
            pltpu.VMEM((parts, own_neg, width), BF16),
            pltpu.VMEM((nodes, width), F32),
            pltpu.SemaphoreType.DMA((parts,)),
            pltpu.SemaphoreType.DMA((parts,)),
            pltpu.SemaphoreType.DMA((chips,)),
            pltpu.SemaphoreType.DMA((chips,)),
        ],
    )(embedding, pairs, degree, my_negs, my_lefts, tile_count, edge_ends[0])
    terms = relations + 1
    orders = layout(parts)
    colors = [orders[color % 2] for color in range(width // LANES)]
    block, neg_block = (terms, width // parts, LANES), (own_neg, LANES)
    outs, scratch = [], []
    for tail, kind in ((block, jnp.int16), ((1, LANES), F32), (neg_block, BF16)):
        outs += [shape((2, *sizes(axes), *tail), kind) for axes in colors]
    outs += [shape((2, *lefts.shape), BF16), shape((2, LANES), F32)]
    for lead in ((2,), ()):
        for tail in (block, neg_block):
            scratch += [pltpu.VMEM((*lead, *sizes(axes), *tail), F32) for axes in colors]
    for tail in (block, neg_block):
        for axes in colors:
            scratch += [pltpu.VMEM((*sizes(axes)[phase:], *tail), F32) for phase in range(3)]
    for inbound in (False, True):
        for tail in (block, neg_block):
            for axes in colors:
                dims = sizes(axes)
                scratch += [pltpu.VMEM((dims[phase] - 1, *dims[phase + 1 :], *tail), jnp.int16) for phase in range(3)]
        for axes in colors:
            scratch += [pltpu.VMEM((size if inbound else size - 1, 8, LANES), F32) for size in sizes(axes)]
    scratch.append(pltpu.VMEM((8, LANES), F32))
    copies = 2 + sum(5 + 6 * sum(size - 1 for size in sizes(axes)) for axes in colors)
    scratch += [pltpu.SemaphoreType.DMA((copies,)), pltpu.SemaphoreType.DMA((copies,))]
    reduced = call(
        functools.partial(reduce_kernel, colors),
        tuple(outs),
        whole(6) + [smem],
        collective=2,
        scratch_shapes=scratch,
    )(features, means, node_grad, neg_grad, lefts, stats, neg_ids)
    gathered, (lefts, total) = reduced[:-2], reduced[-2:]
    weight_grad, loss, pre_grad = pl.pallas_call(
        functools.partial(finish_kernel, colors),
        grid=(terms,),
        out_shape=(shape((terms, width, width), F32), shape((1, LANES), F32), shape((nodes, width), BF16)),
        in_specs=[smem] + whole(3 + len(gathered)),
        out_specs=(
            pl.BlockSpec((1, width, width), lambda term: (term, 0, 0)),
            pl.BlockSpec((1, LANES), lambda term: (0, 0)),
            pl.BlockSpec((nodes, width), lambda term: (0, 0)),
        ),
        scratch_shapes=[pltpu.VMEM((parts * own_neg, width), BF16)],
        compiler_params=pltpu.CompilerParams(vmem_limit_bytes=VMEM_LIMIT),
    )(neg_ids, pre, lefts, total, *gathered)
    return (weight_grad, loss[0, 0], pre_grad)


def solution(mesh):
    placed = (
        P("dom", None),
        P(),
        P("dom", None, None),
        P("dom", None, None),
        P("dom"),
        P("dom", None, None),
        P("dom"),
    )
    return jax.shard_map(
        functools.partial(on_device, mesh.shape["dom"]),
        mesh=mesh,
        in_specs=placed,
        out_specs=(P(), P(), P("dom", None)),
        check_vma=False,
    )
```

```python
import functools
import itertools

import jax
import jax.numpy as jnp
from jax import lax
from jax.experimental import pallas as pl
from jax.experimental.pallas import tpu as pltpu
from jax.sharding import PartitionSpec as P

F32 = jnp.float32
BF16 = jnp.bfloat16
VMEM_LIMIT = 48 * 1024 * 1024
LANES = 128
STEPS = 32700.0
TINY = 1e-30
MESH = pl.DeviceIdType.MESH


def whole(count):
    return [pl.BlockSpec(memory_space=pltpu.VMEM)] * count


def nn(a, b):
    return jnp.dot(a, b, preferred_element_type=F32)


def nt(a, b):
    return lax.dot_general(a, b, (((1,), (1,)), ((), ())), preferred_element_type=F32)


def tn(a, b):
    return lax.dot_general(a, b, (((0,), (0,)), ((), ())), preferred_element_type=F32)


def halves(x):
    high = x.astype(BF16)
    return high, (x - high.astype(F32)).astype(BF16)


def one_hot(mask):
    return jnp.where(mask, 1.0, 0.0).astype(BF16)


def build_table(fan, nbr_ref, table_ref):
    nodes, slots = table_ref.shape[1:]
    step = 64

    @pl.loop(0, nodes // step)
    def _(block):
        rows = pl.ds(pl.multiple_of(block * step, step), step)
        lanes = lax.broadcasted_iota(jnp.int32, (step, slots), 1)
        named = nbr_ref[rows, :]
        for relation in range(table_ref.shape[0]):
            total = jnp.zeros((step, slots), F32)
            for k in range(fan):
                column = relation * fan + k
                total = total + jnp.where(named[:, column : column + 1] == lanes, 1.0, 0.0)
            table_ref[relation, rows, :] = total.astype(BF16)


def build_pairs(ends_ref, count_ref, source_ref, target_ref):
    tiles, _, tile = ends_ref.shape
    nodes = source_ref.shape[0]
    step = 128

    @pl.loop(0, tiles)
    def _(at):
        ends = jnp.where(at < count_ref[0], ends_ref[at], -1)
        lanes = pl.ds(pl.multiple_of(at * tile, tile), tile)
        for block in range(0, nodes, step):
            rows = lax.broadcasted_iota(jnp.int32, (step, tile), 0) + block
            source_ref[block : block + step, lanes] = one_hot(ends[0:1, :] == rows)
            target_ref[block : block + step, lanes] = one_hot(ends[1:2, :] == rows)


def front(
    fan, feat_hbm, weights_hbm, nbr_ref, halo_ref, ends_ref, count_ref, ids_ref,
    own_ref, means_ref, grad_ref, pre_ref, neg_ref, stats_ref,
    weights_ref, table_ref, part_ref, first_ref, source_ref, target_ref, pairs_ref, embed_ref,
    halo_out, halo_in, mine_ref, landed, left_ref, lefts_ref, load_sem, send_sem, recv_sem,
):
    parts, per_peer = halo_ref.shape
    nodes, width = own_ref.shape
    relations = table_ref.shape[0]
    own_neg = ids_ref.shape[0]
    me = lax.axis_index("dom")
    core, place, chips = me % 2, me // 2, parts // 2
    loads = [
        pltpu.make_async_copy(feat_hbm, own_ref, load_sem.at[0]),
        pltpu.make_async_copy(weights_hbm, weights_ref, load_sem.at[1]),
    ]
    for load in loads:
        load.start()
    barrier = pltpu.get_barrier_semaphore()

    @pl.loop(1, parts)
    def _(i):
        pl.semaphore_signal(barrier, inc=1, device_id=((me + i) % parts,), device_id_type=MESH)

    def remote(source, target, kind, sem, slot, peer):
        return pltpu.make_async_remote_copy(
            src_ref=source,
            dst_ref=target,
            send_sem=send_sem.at[kind, sem],
            recv_sem=recv_sem.at[kind, slot],
            device_id=(peer,),
            device_id_type=MESH,
        )

    def halo_to(peer, slot, sem):
        return remote(halo_out.at[peer], halo_in.at[slot], 0, sem, slot, peer)

    def neg_to(peer, slot, sem):
        return remote(mine_ref, landed.at[slot], 1, sem, slot, peer)

    def left_to(other, slot, sem):
        return remote(left_ref, lefts_ref.at[slot], 2, sem, slot, 2 * other + core)

    asked = parts * per_peer
    spread = lax.broadcasted_iota(jnp.int32, (asked, parts), 0) // per_peer
    spread = jnp.where(spread == lax.broadcasted_iota(jnp.int32, (asked, parts), 1), 1.0, 0.0)
    wanted = jnp.dot(spread, halo_ref[...].astype(F32), preferred_element_type=F32, precision=lax.Precision.HIGHEST)
    slot_of = lax.broadcasted_iota(jnp.int32, (asked, per_peer), 0) % per_peer
    wanted = jnp.where(slot_of == lax.broadcasted_iota(jnp.int32, (asked, per_peer), 1), wanted, 0.0)
    wanted = jnp.sum(wanted, axis=1, keepdims=True)
    lanes = lax.broadcasted_iota(jnp.int32, (asked, nodes), 1).astype(F32)
    wanted = one_hot(wanted == lanes)
    loads[0].wait()
    halo_out[...] = nn(wanted, own_ref[...]).reshape(parts, per_peer, width).astype(BF16)
    pl.semaphore_wait(barrier, parts - 1)

    @pl.loop(1, parts)
    def _(i):
        halo_to((me + i) % parts, me, i).start()

    halo_in[me] = halo_out[me]
    build_table(fan, nbr_ref, table_ref)
    own = own_ref[...]
    for relation in range(relations):
        part_ref[relation] = nn(table_ref[relation, :, :nodes], own)
    loads[1].wait()
    first_ref[...] = nn(own, weights_ref[0])

    @pl.loop(1, parts)
    def _(i):
        halo_to((me + i) % parts, (me + i) % parts, i).wait()

    halo = halo_in[...].reshape(asked, width)
    preact = first_ref[...]
    for relation in range(relations):
        mean = ((part_ref[relation] + nn(table_ref[relation, :, nodes:], halo)) / fan).astype(BF16)
        means_ref[relation] = mean
        preact = preact + nn(mean, weights_ref[relation + 1])
    embedding = preact.astype(BF16)
    embed_ref[...] = embedding
    lanes = lax.broadcasted_iota(jnp.int32, (own_neg, nodes), 1)
    slot, ids = id_column(ids_ref)
    mine_ref[...] = nn(one_hot(ids == lanes), embedding).astype(BF16)

    @pl.loop(1, parts)
    def _(i):
        neg_to((me + i) % parts, me, i).start()

    again = jnp.zeros_like(ids)
    for j in range(own_neg):
        again = again + jnp.where((ids == ids_ref[j]) & (slot > j), 1, 0)
    pick = one_hot((ids == lanes) & (again == 0))
    left_ref[0] = nn(pick, own).astype(BF16)
    for relation in range(relations):
        left_ref[relation + 1] = nn(pick, means_ref[relation]).astype(BF16)

    @pl.loop(1, chips)
    def _(i):
        left_to((place + i) % chips, place, i).start()

    landed[me] = mine_ref[...]
    lefts_ref[place] = left_ref[...]
    build_pairs(ends_ref, count_ref, source_ref, target_ref)
    pairs = nt(source_ref[...], target_ref[...])
    degree = jnp.sum(pairs, axis=1, keepdims=True)
    pairs_ref[...] = pairs + pairs.T
    pairs = pairs_ref[...]
    embedding = embed_ref[...]
    score = nt(embedding, embedding)
    small = jnp.exp(-jnp.abs(score))
    positive_loss = 0.5 * jnp.sum(pairs * (jnp.maximum(-score, 0.0) + jnp.log1p(small)))
    high, low = halves(-pairs * (jnp.where(score >= 0, small, 1.0) / (1.0 + small)))
    grad_ref[...] = nn(high, embedding) + nn(low, embedding)

    @pl.loop(1, parts)
    def _(i):
        neg_to((me + i) % parts, (me + i) % parts, i).wait()

    negatives = landed[...].reshape(parts * own_neg, width)
    count = negatives.shape[0]
    score = nt(embedding, negatives)
    small = jnp.exp(-jnp.abs(score))
    loss = jnp.maximum(score, 0.0) + jnp.log1p(small)
    loss_sum = positive_loss + jnp.sum(degree * loss) / count
    slope = ((jnp.where(score >= 0, 1.0, small) / (1.0 + small)) / count).astype(BF16)
    grad = grad_ref[...] + degree * nn(slope, negatives)
    grad_ref[...] = grad
    pre_ref[...] = grad.astype(BF16)
    high, low = halves(degree * embedding.astype(F32))
    neg_ref[...] = tn(slope, high) + tn(slope, low)
    edges = count_ref[0].astype(F32) * ends_ref.shape[2]
    rows = lax.broadcasted_iota(jnp.int32, stats_ref.shape, 0)
    stats_ref[...] = jnp.where(rows == 2, loss_sum, edges)

    def lefts_wait():
        @pl.loop(1, chips)
        def _(i):
            left_to((place + i) % chips, (place + i) % chips, i).wait()

    return lefts_wait


def layout(parts):
    radix = [1, 1, 1]
    at = 0
    while radix[0] * radix[1] * radix[2] * 2 < parts:
        radix[at % 3] *= 2
        at += 1
    outer, middle, inner = radix
    first, second, last = (inner, 2), (middle, 2 * inner), (outer, 2 * inner * middle)
    return [[first, second, last], [second, first, last]]


def sizes(axes):
    return tuple(size for size, _ in axes)


def device_of(axes, core, spot):
    return core + sum(at * stride for at, (_, stride) in zip(spot, axes))


def spots_of(axes):
    return itertools.product(*(range(size) for size, _ in axes))


def id_column(ids_ref):
    count = ids_ref.shape[0]
    rows = lax.broadcasted_iota(jnp.int32, (count, 1), 0)
    column = jnp.zeros((count, 1), jnp.int32)
    for j in range(count):
        column = jnp.where(rows == j, ids_ref[j], column)
    return rows, column


def quantize(x, scale):
    return jnp.round(x * (1.0 / scale)).astype(jnp.int32).astype(jnp.int16)


def lane_scale(x):
    top = jnp.max(jnp.abs(x).reshape(-1, x.shape[-1]), axis=0, keepdims=True)
    return jnp.maximum(top, TINY) * (1.0 / STEPS)


def step_kernel(colors, fan, feat_hbm, weights_hbm, nbr_ref, halo_ref, ends_ref, count_ref, ids_ref, *refs):
    count = len(colors)
    me = lax.axis_index("dom")
    core = me % 2
    partner = me + 1 - 2 * core
    refs = list(refs)

    def take(number):
        taken = refs[:number]
        del refs[:number]
        return taken

    words, scales, rows_out = take(count), take(count), take(count)
    lefts_out, total_ref, pre_ref = take(3)
    own_ref, means_ref, grad_ref, neg_ref, stats_ref = take(5)
    inner = take(17)
    lefts_ref = inner[13]
    terms = means_ref.shape[0] + 1
    lefts_wait = front(
        fan, feat_hbm, weights_hbm, nbr_ref, halo_ref, ends_ref, count_ref, ids_ref,
        own_ref, means_ref, grad_ref, pre_ref, neg_ref, stats_ref, *inner,
    )
    full, full_neg, paired, paired_neg = take(count), take(count), take(count), take(count)
    sums, sums_neg = [take(3) for _ in colors], [take(3) for _ in colors]
    out_q, out_n, out_m = [take(3) for _ in colors], [take(3) for _ in colors], [take(3) for _ in colors]
    in_q, in_n, in_m = [take(3) for _ in colors], [take(3) for _ in colors], [take(3) for _ in colors]
    stats_in, send_sem, recv_sem = take(3)
    spots = {}

    def remote(source, target, key, peer):
        at = spots.setdefault(key, len(spots))
        return pltpu.make_async_remote_copy(
            src_ref=source,
            dst_ref=target,
            send_sem=send_sem.at[at],
            recv_sem=recv_sem.at[at],
            device_id=(peer,),
            device_id_type=MESH,
        )

    def mine(axis):
        size, stride = axis
        return (me // stride) % size

    stats_copy = remote(stats_ref, stats_in, "stats", partner)
    stats_copy.start()

    nodes, width = grad_ref.shape
    own_neg = ids_ref.shape[0]
    slot, ids = id_column(ids_ref)
    node = lax.broadcasted_iota(jnp.int32, (nodes, 1), 0)
    named = jnp.zeros((nodes, 1), jnp.bool_)
    for j in range(own_neg):
        named = named | (node == ids_ref[j])
    pre = jnp.where(named, 0.0, grad_ref[...]).astype(BF16)
    lanes = lax.broadcasted_iota(jnp.int32, (own_neg, nodes), 1)
    pick = jnp.where(ids == lanes, 1.0, 0.0)
    local = jnp.dot(pick, grad_ref[...], preferred_element_type=F32, precision=lax.Precision.HIGHEST)
    rows = full[0].shape[5]
    pairs = []
    wide = 2 * LANES
    for half in range(0, count, 2):
        lanes = slice(half * LANES, half * LANES + wide)
        for color in (half, half + 1):
            axes = colors[color]
            for c in range(2):
                for spot in spots_of(axes):
                    at = device_of(axes, c, spot) * own_neg
                    full_neg[color][(c, *spot)] = neg_ref[at : at + own_neg, color * LANES : (color + 1) * LANES]
        for term in range(terms):
            left = own_ref[...] if term == 0 else means_ref[term - 1]
            product = tn(left, pre[:, lanes])
            for color in (half, half + 1):
                axes = colors[color]
                part = product[:, (color - half) * LANES : (color - half + 1) * LANES]
                for c in range(2):
                    for spot in spots_of(axes):
                        at = device_of(axes, c, spot) * rows
                        full[color][(c, *spot, term)] = part[at : at + rows]
        for color in (half, half + 1):
            pairs.append([
                remote(full[color].at[1 - core], paired[color], ("pair", color), partner),
                remote(full_neg[color].at[1 - core], paired_neg[color], ("pair_neg", color), partner),
            ])
            for copy in pairs[-1]:
                copy.start()

    def scatter(color, phase, stats):
        axis = colors[color][phase]
        size, stride = axis
        at = mine(axis)
        copies = []
        for delta in range(1, size):
            other = (at + delta) % size
            peer = me + (other - at) * stride
            block, neg = sums[color][phase][other], sums_neg[color][phase][other]
            scale, neg_scale = lane_scale(block), lane_scale(neg)
            spot = delta - 1
            out_q[color][phase][spot] = quantize(block, scale)
            out_n[color][phase][spot] = quantize(neg, neg_scale)
            out_m[color][phase][spot, 0:1] = scale
            out_m[color][phase][spot, 1:2] = neg_scale
            out_m[color][phase][spot, 2:4] = stats
            key = ("scatter", color, phase, delta)
            copies += [
                remote(out_q[color][phase].at[spot], in_q[color][phase].at[spot], (*key, 0), peer),
                remote(out_n[color][phase].at[spot], in_n[color][phase].at[spot], (*key, 1), peer),
                remote(out_m[color][phase].at[spot], in_m[color][phase].at[at], (*key, 2), peer),
            ]
        for copy in copies:
            copy.start()
        return copies

    def gather(color, phase):
        axes = colors[color]
        at = [mine(axis) for axis in axes]
        index = (core, *at[: phase + 1])
        copies = []
        if phase < 0:
            for kind, ref in enumerate((words[color], scales[color], rows_out[color])):
                copies.append(remote(ref.at[core], ref.at[core], ("gather", color, phase, 0, kind), partner))
        else:
            size, stride = axes[phase]
            for delta in range(1, size):
                peer = me + ((at[phase] + delta) % size - at[phase]) * stride
                for kind, ref in enumerate((words[color], scales[color], rows_out[color])):
                    copies.append(remote(ref.at[index], ref.at[index], ("gather", color, phase, delta, kind), peer))
        for copy in copies:
            copy.start()
        return copies

    stats_copy.wait()
    stats = [None] * count
    stats[0] = stats_ref[2:4] + stats_in[2:4]
    for color in range(1, count):
        stats[color] = stats[0]
    flying = []
    for color in range(count):
        for copy in pairs[color]:
            copy.wait()
        sums[color][0][...] = full[color][core] + paired[color][...]
        sums_neg[color][0][...] = full_neg[color][core] + paired_neg[color][...]
        flying.append(scatter(color, 0, stats[color]))
    lefts_wait()
    lefts_copy = remote(lefts_ref, lefts_out.at[core], "lefts", partner)
    lefts_copy.start()
    lefts_out[core] = lefts_ref[...]
    for phase in range(3):
        for color in range(count):
            axis = colors[color][phase]
            size = axis[0]
            at = mine(axis)
            for copy in flying[color]:
                copy.wait()
            total = sums[color][phase][at]
            total_neg = sums_neg[color][phase][at]
            for delta in range(1, size):
                meta = in_m[color][phase][(at + size - delta) % size]
                total = total + in_q[color][phase][delta - 1].astype(jnp.int32).astype(F32) * meta[0:1]
                total_neg = total_neg + in_n[color][phase][delta - 1].astype(jnp.int32).astype(F32) * meta[1:2]
            in_m[color][phase][at, 2:4] = stats[color]
            stats[color] = in_m[color][phase][0, 2:4]
            for position in range(1, size):
                stats[color] = stats[color] + in_m[color][phase][position, 2:4]
            if phase < 2:
                sums[color][phase + 1][...] = total
                sums_neg[color][phase + 1][...] = total_neg
                flying[color] = scatter(color, phase + 1, stats[color])
            else:
                index = (core, *(mine(a) for a in colors[color]))
                scale = lane_scale(total)
                words[color][index] = quantize(total, scale)
                scales[color][index] = scale
                gathered = local[:, color * LANES : (color + 1) * LANES]
                for j in range(own_neg):
                    gathered = gathered + jnp.where(ids == ids_ref[j], total_neg[j : j + 1], 0.0)
                rows_out[color][index] = gathered.astype(BF16)
                flying[color] = gather(color, 2)
    total_ref[0:2] = stats[0]
    for phase in (1, 0, -1):
        for color in range(count):
            for copy in flying[color]:
                copy.wait()
            flying[color] = gather(color, phase)
    for color in range(count):
        for copy in flying[color]:
            copy.wait()
    lefts_copy.wait()


def finish_kernel(colors, ids_ref, pre_ref, lefts_ref, total_ref, *refs):
    count = len(colors)
    words, scales, rows_in = refs[:count], refs[count : 2 * count], refs[2 * count : 3 * count]
    out_ref, loss_ref, pre_out, joint = refs[3 * count :]
    term = pl.program_id(0)
    own_neg = ids_ref.shape[0]
    chips = lefts_ref.shape[1]
    edges = total_ref[1:2]
    inverse = 1.0 / edges

    @pl.when(term == 0)
    def _():
        me = lax.axis_index("dom")
        loss_ref[...] = total_ref[0:1] / edges
        for color, axes in enumerate(colors):
            for c in range(2):
                for spot in spots_of(axes):
                    at = (c * chips + device_of(axes, 0, spot) // 2) * own_neg
                    joint[at : at + own_neg, color * LANES : (color + 1) * LANES] = rows_in[color][(c, *spot)]
        slot, ids = id_column(ids_ref)
        again = jnp.zeros_like(ids)
        for j in range(own_neg):
            again = again + jnp.where((ids == ids_ref[j]) & (slot > j), 1, 0)
        nodes = pre_ref.shape[0]
        lanes = lax.broadcasted_iota(jnp.int32, (own_neg, nodes), 1)
        pick = one_hot((ids == lanes) & (again == 0))
        node = lax.broadcasted_iota(jnp.int32, (nodes, 1), 0)
        named = jnp.zeros((nodes, 1), jnp.bool_)
        for j in range(own_neg):
            named = named | (node == ids_ref[j])
        for color, axes in enumerate(colors):
            block = slice(color * LANES, (color + 1) * LANES)
            index = (me % 2, *((me // stride) % size for size, stride in axes))
            patch = tn(pick, rows_in[color][index])
            pre_out[:, block] = jnp.where(named, patch, pre_ref[:, block].astype(F32)).astype(BF16)

    lefts = lefts_ref[:, :, term].reshape(2 * chips * own_neg, lefts_ref.shape[4])
    extra = tn(lefts, joint[...])
    rows = words[0].shape[5]
    for color, axes in enumerate(colors):
        block = slice(color * LANES, (color + 1) * LANES)
        for c in range(2):
            for spot in spots_of(axes):
                at = device_of(axes, c, spot) * rows
                value = words[color][(c, *spot, term)].astype(jnp.int32).astype(F32) * scales[color][(c, *spot)]
                out_ref[0, at : at + rows, block] = (value + extra[at : at + rows, block]) * inverse


def call(kernel, out_shape, in_specs, collective=None, **kwargs):
    extra = {} if collective is None else {"collective_id": collective, "has_side_effects": True}
    many = isinstance(out_shape, (list, tuple))
    return pl.pallas_call(
        kernel,
        out_shape=out_shape,
        in_specs=in_specs,
        out_specs=whole(len(out_shape)) if many else whole(1)[0],
        compiler_params=pltpu.CompilerParams(vmem_limit_bytes=VMEM_LIMIT, **extra),
        **kwargs,
    )


def shape(dims, kind):
    return jax.ShapeDtypeStruct(dims, kind)


def on_device(parts, features, weights, halo_send, nbr_index, tile_count, edge_ends, neg_ids):
    nodes, width = features.shape
    relations, fan = nbr_index.shape[1:]
    per_peer = halo_send.shape[2]
    slots = nodes + parts * per_peer
    own_neg = neg_ids.shape[0]
    smem = pl.BlockSpec(memory_space=pltpu.SMEM)
    hbm = pl.BlockSpec(memory_space=pl.ANY)
    chips = parts // 2
    terms = relations + 1
    edges = edge_ends.shape[0] * edge_ends.shape[2]
    orders = layout(parts)
    colors = [orders[color % 2] for color in range(width // LANES)]
    block, neg_block = (terms, width // parts, LANES), (own_neg, LANES)
    outs, scratch = [], []
    for tail, kind in ((block, jnp.int16), ((1, LANES), F32), (neg_block, BF16)):
        outs += [shape((2, *sizes(axes), *tail), kind) for axes in colors]
    outs += [
        shape((2, chips, terms, own_neg, width), BF16),
        shape((2, LANES), F32),
        shape((nodes, width), BF16),
    ]
    scratch += [
        pltpu.VMEM((nodes, width), BF16),
        pltpu.VMEM((relations, nodes, width), BF16),
        pltpu.VMEM((nodes, width), F32),
        pltpu.VMEM((parts * own_neg, width), F32),
        pltpu.VMEM((8, LANES), F32),
        pltpu.VMEM(weights.shape, BF16),
        pltpu.VMEM((relations, nodes, slots), BF16),
        pltpu.VMEM((relations, nodes, width), F32),
        pltpu.VMEM((nodes, width), F32),
        pltpu.VMEM((nodes, edges), BF16),
        pltpu.VMEM((nodes, edges), BF16),
        pltpu.VMEM((nodes, nodes), F32),
        pltpu.VMEM((nodes, width), BF16),
        pltpu.VMEM((parts, per_peer, width), BF16),
        pltpu.VMEM((parts, per_peer, width), BF16),
        pltpu.VMEM((own_neg, width), BF16),
        pltpu.VMEM((parts, own_neg, width), BF16),
        pltpu.VMEM((terms, own_neg, width), BF16),
        pltpu.VMEM((chips, terms, own_neg, width), BF16),
        pltpu.SemaphoreType.DMA((2,)),
        pltpu.SemaphoreType.DMA((3, parts)),
        pltpu.SemaphoreType.DMA((3, parts)),
    ]
    for lead in ((2,), ()):
        for tail in (block, neg_block):
            scratch += [pltpu.VMEM((*lead, *sizes(axes), *tail), F32) for axes in colors]
    for tail in (block, neg_block):
        for axes in colors:
            scratch += [pltpu.VMEM((*sizes(axes)[phase:], *tail), F32) for phase in range(3)]
    for inbound in (False, True):
        for tail in (block, neg_block):
            for axes in colors:
                dims = sizes(axes)
                scratch += [pltpu.VMEM((dims[phase] - 1, *dims[phase + 1 :], *tail), jnp.int16) for phase in range(3)]
        for axes in colors:
            scratch += [pltpu.VMEM((size if inbound else size - 1, 8, LANES), F32) for size in sizes(axes)]
    scratch.append(pltpu.VMEM((8, LANES), F32))
    copies = 2 + sum(5 + 6 * sum(size - 1 for size in sizes(axes)) for axes in colors)
    scratch += [pltpu.SemaphoreType.DMA((copies,)), pltpu.SemaphoreType.DMA((copies,))]
    reduced = call(
        functools.partial(step_kernel, colors, fan),
        tuple(outs),
        [hbm, hbm] + whole(3) + [smem, smem],
        collective=2,
        scratch_shapes=scratch,
    )(features, weights, nbr_index.reshape(nodes, relations * fan), halo_send[0], edge_ends, tile_count, neg_ids)
    gathered, (lefts, total, pre) = reduced[:-3], reduced[-3:]
    weight_grad, loss, pre_grad = pl.pallas_call(
        functools.partial(finish_kernel, colors),
        grid=(terms,),
        out_shape=(shape((terms, width, width), F32), shape((1, LANES), F32), shape((nodes, width), BF16)),
        in_specs=[smem] + whole(3 + len(gathered)),
        out_specs=(
            pl.BlockSpec((1, width, width), lambda term: (term, 0, 0)),
            pl.BlockSpec((1, LANES), lambda term: (0, 0)),
            pl.BlockSpec((nodes, width), lambda term: (0, 0)),
        ),
        scratch_shapes=[pltpu.VMEM((parts * own_neg, width), BF16)],
        compiler_params=pltpu.CompilerParams(vmem_limit_bytes=VMEM_LIMIT),
    )(neg_ids, pre, lefts, total, *gathered)
    return (weight_grad, loss[0, 0], pre_grad)


def solution(mesh):
    placed = (
        P("dom", None),
        P(),
        P("dom", None, None),
        P("dom", None, None),
        P("dom"),
        P("dom", None, None),
        P("dom"),
    )
    return jax.shard_map(
        functools.partial(on_device, mesh.shape["dom"]),
        mesh=mesh,
        in_specs=placed,
        out_specs=(P(), P(), P("dom", None)),
        check_vma=False,
    )
```

```python
import functools
import itertools

import jax
import jax.numpy as jnp
from jax import lax
from jax.experimental import pallas as pl
from jax.experimental.pallas import tpu as pltpu
from jax.sharding import PartitionSpec as P

F32 = jnp.float32
BF16 = jnp.bfloat16
VMEM_LIMIT = 48 * 1024 * 1024
LANES = 128
STEPS = 32700.0
TINY = 1e-30
MESH = pl.DeviceIdType.MESH


def whole(count):
    return [pl.BlockSpec(memory_space=pltpu.VMEM)] * count


def nn(a, b):
    return jnp.dot(a, b, preferred_element_type=F32)


def nt(a, b):
    return lax.dot_general(a, b, (((1,), (1,)), ((), ())), preferred_element_type=F32)


def tn(a, b):
    return lax.dot_general(a, b, (((0,), (0,)), ((), ())), preferred_element_type=F32)


def halves(x):
    high = x.astype(BF16)
    return high, (x - high.astype(F32)).astype(BF16)


def one_hot(mask):
    return jnp.where(mask, 1.0, 0.0).astype(BF16)


def build_table(fan, nbr_ref, table_ref):
    nodes, slots = table_ref.shape[1:]
    step = 64

    @pl.loop(0, nodes // step)
    def _(block):
        rows = pl.ds(pl.multiple_of(block * step, step), step)
        lanes = lax.broadcasted_iota(jnp.int32, (step, slots), 1)
        named = nbr_ref[rows, :]
        for relation in range(table_ref.shape[0]):
            total = jnp.zeros((step, slots), F32)
            for k in range(fan):
                column = relation * fan + k
                total = total + jnp.where(named[:, column : column + 1] == lanes, 1.0, 0.0)
            table_ref[relation, rows, :] = total.astype(BF16)


def build_pairs(ends_ref, count_ref, source_ref, target_ref):
    tiles, _, tile = ends_ref.shape
    nodes = source_ref.shape[0]
    step = 128

    @pl.loop(0, tiles)
    def _(at):
        ends = jnp.where(at < count_ref[0], ends_ref[at], -1)
        lanes = pl.ds(pl.multiple_of(at * tile, tile), tile)
        for block in range(0, nodes, step):
            rows = lax.broadcasted_iota(jnp.int32, (step, tile), 0) + block
            source_ref[block : block + step, lanes] = one_hot(ends[0:1, :] == rows)
            target_ref[block : block + step, lanes] = one_hot(ends[1:2, :] == rows)


def front(
    fan, inputs, count_ref, ids_ref, own_ref, means_ref, grad_ref, pre_ref, neg_ref, stats_ref,
    weights_ref, nbr_in, nbr_ref, halo_ref, ends_ref, table_ref, part_ref, first_ref, source_ref, target_ref, pairs_ref, embed_ref,
    halo_out, halo_in, mine_ref, landed, left_ref, lefts_ref, load_sem, send_sem, recv_sem,
):
    per_peer, parts = halo_ref.shape
    nodes, width = own_ref.shape
    relations = table_ref.shape[0]
    own_neg = ids_ref.shape[0]
    me = lax.axis_index("dom")
    core, place, chips = me % 2, me // 2, parts // 2
    targets = (halo_ref, own_ref, nbr_in, weights_ref, ends_ref, ids_ref)
    loads = [pltpu.make_async_copy(*pair, load_sem.at[at]) for at, pair in enumerate(zip(inputs, targets))]
    for load in loads:
        load.start()
    barrier = pltpu.get_barrier_semaphore()

    @pl.loop(1, parts)
    def _(i):
        pl.semaphore_signal(barrier, inc=1, device_id=((me + i) % parts,), device_id_type=MESH)

    def remote(source, target, kind, sem, slot, peer):
        return pltpu.make_async_remote_copy(
            src_ref=source,
            dst_ref=target,
            send_sem=send_sem.at[kind, sem],
            recv_sem=recv_sem.at[kind, slot],
            device_id=(peer,),
            device_id_type=MESH,
        )

    def halo_to(peer, slot, sem):
        return remote(halo_out.at[peer], halo_in.at[slot], 0, sem, slot, peer)

    def neg_to(peer, slot, sem):
        return remote(mine_ref, landed.at[slot], 1, sem, slot, peer)

    def left_to(other, slot, sem):
        return remote(left_ref, lefts_ref.at[slot], 2, sem, slot, 2 * other + core)

    asked = parts * per_peer
    spread = lax.broadcasted_iota(jnp.int32, (asked, parts), 0) // per_peer
    spread = jnp.where(spread == lax.broadcasted_iota(jnp.int32, (asked, parts), 1), 1.0, 0.0)
    loads[0].wait()
    wanted = lax.dot_general(
        spread,
        halo_ref[...].astype(F32),
        (((1,), (1,)), ((), ())),
        preferred_element_type=F32,
        precision=lax.Precision.HIGHEST,
    )
    slot_of = lax.broadcasted_iota(jnp.int32, (asked, per_peer), 0) % per_peer
    wanted = jnp.where(slot_of == lax.broadcasted_iota(jnp.int32, (asked, per_peer), 1), wanted, 0.0)
    wanted = jnp.sum(wanted, axis=1, keepdims=True)
    lanes = lax.broadcasted_iota(jnp.int32, (asked, nodes), 1).astype(F32)
    wanted = one_hot(wanted == lanes)
    loads[1].wait()
    halo_out[...] = nn(wanted, own_ref[...]).reshape(parts, per_peer, width).astype(BF16)
    pl.semaphore_wait(barrier, parts - 1)

    @pl.loop(1, parts)
    def _(i):
        halo_to((me + i) % parts, me, i).start()

    halo_in[me] = halo_out[me]
    loads[2].wait()
    nbr_ref[...] = nbr_in[...].T
    build_table(fan, nbr_ref, table_ref)
    own = own_ref[...]
    for relation in range(relations):
        part_ref[relation] = nn(table_ref[relation, :, :nodes], own)
    loads[3].wait()
    first_ref[...] = nn(own, weights_ref[0])

    @pl.loop(1, parts)
    def _(i):
        halo_to((me + i) % parts, (me + i) % parts, i).wait()

    halo = halo_in[...].reshape(asked, width)
    preact = first_ref[...]
    for relation in range(relations):
        mean = ((part_ref[relation] + nn(table_ref[relation, :, nodes:], halo)) / fan).astype(BF16)
        means_ref[relation] = mean
        preact = preact + nn(mean, weights_ref[relation + 1])
    embedding = preact.astype(BF16)
    embed_ref[...] = embedding
    lanes = lax.broadcasted_iota(jnp.int32, (own_neg, nodes), 1)
    loads[5].wait()
    slot, ids = id_column(ids_ref)
    mine_ref[...] = nn(one_hot(ids == lanes), embedding).astype(BF16)

    @pl.loop(1, parts)
    def _(i):
        neg_to((me + i) % parts, me, i).start()

    again = jnp.zeros_like(ids)
    for j in range(own_neg):
        again = again + jnp.where((ids == ids_ref[j]) & (slot > j), 1, 0)
    pick = one_hot((ids == lanes) & (again == 0))
    left_ref[0] = nn(pick, own).astype(BF16)
    for relation in range(relations):
        left_ref[relation + 1] = nn(pick, means_ref[relation]).astype(BF16)

    @pl.loop(1, chips)
    def _(i):
        left_to((place + i) % chips, place, i).start()

    landed[me] = mine_ref[...]
    lefts_ref[place] = left_ref[...]
    loads[4].wait()
    build_pairs(ends_ref, count_ref, source_ref, target_ref)
    pairs = nt(source_ref[...], target_ref[...])
    degree = jnp.sum(pairs, axis=1, keepdims=True)
    pairs_ref[...] = pairs + pairs.T
    pairs = pairs_ref[...]
    embedding = embed_ref[...]
    score = nt(embedding, embedding)
    small = jnp.exp(-jnp.abs(score))
    positive_loss = 0.5 * jnp.sum(pairs * (jnp.maximum(-score, 0.0) + jnp.log1p(small)))
    high, low = halves(-pairs * (jnp.where(score >= 0, small, 1.0) / (1.0 + small)))
    grad_ref[...] = nn(high, embedding) + nn(low, embedding)

    @pl.loop(1, parts)
    def _(i):
        neg_to((me + i) % parts, (me + i) % parts, i).wait()

    negatives = landed[...].reshape(parts * own_neg, width)
    count = negatives.shape[0]
    score = nt(embedding, negatives)
    small = jnp.exp(-jnp.abs(score))
    loss = jnp.maximum(score, 0.0) + jnp.log1p(small)
    loss_sum = positive_loss + jnp.sum(degree * loss) / count
    slope = ((jnp.where(score >= 0, 1.0, small) / (1.0 + small)) / count).astype(BF16)
    grad = grad_ref[...] + degree * nn(slope, negatives)
    grad_ref[...] = grad
    pre_ref[...] = grad.astype(BF16)
    high, low = halves(degree * embedding.astype(F32))
    neg_ref[...] = tn(slope, high) + tn(slope, low)
    edges = count_ref[0].astype(F32) * ends_ref.shape[2]
    rows = lax.broadcasted_iota(jnp.int32, stats_ref.shape, 0)
    stats_ref[...] = jnp.where(rows == 2, loss_sum, edges)

    def lefts_wait():
        @pl.loop(1, chips)
        def _(i):
            left_to((place + i) % chips, (place + i) % chips, i).wait()

    return lefts_wait


def layout(parts):
    radix = [1, 1, 1]
    at = 0
    while radix[0] * radix[1] * radix[2] * 2 < parts:
        radix[at % 3] *= 2
        at += 1
    outer, middle, inner = radix
    first, second, last = (inner, 2), (middle, 2 * inner), (outer, 2 * inner * middle)
    return [[first, second, last], [second, first, last]]


def sizes(axes):
    return tuple(size for size, _ in axes)


def device_of(axes, core, spot):
    return core + sum(at * stride for at, (_, stride) in zip(spot, axes))


def spots_of(axes):
    return itertools.product(*(range(size) for size, _ in axes))


def id_column(ids_ref):
    count = ids_ref.shape[0]
    rows = lax.broadcasted_iota(jnp.int32, (count, 1), 0)
    column = jnp.zeros((count, 1), jnp.int32)
    for j in range(count):
        column = jnp.where(rows == j, ids_ref[j], column)
    return rows, column


def quantize(x, scale):
    return jnp.round(x * (1.0 / scale)).astype(jnp.int32).astype(jnp.int16)


def lane_scale(x):
    top = jnp.max(jnp.abs(x).reshape(-1, x.shape[-1]), axis=0, keepdims=True)
    return jnp.maximum(top, TINY) * (1.0 / STEPS)


def step_kernel(colors, fan, *refs):
    count = len(colors)
    me = lax.axis_index("dom")
    core = me % 2
    partner = me + 1 - 2 * core
    refs = list(refs)

    def take(number):
        taken = refs[:number]
        del refs[:number]
        return taken

    inputs = take(6)
    (count_ref,) = take(1)
    words, scales, rows_out = take(count), take(count), take(count)
    lefts_out, total_ref, pre_ref = take(3)
    ids_ref, own_ref, means_ref, grad_ref, neg_ref, stats_ref = take(6)
    inner = take(21)
    lefts_ref = inner[17]
    terms = means_ref.shape[0] + 1
    lefts_wait = front(
        fan, inputs, count_ref, ids_ref, own_ref, means_ref, grad_ref, pre_ref, neg_ref, stats_ref, *inner,
    )
    full, full_neg, paired, paired_neg = take(count), take(count), take(count), take(count)
    sums, sums_neg = [take(3) for _ in colors], [take(3) for _ in colors]
    out_q, out_n, out_m = [take(3) for _ in colors], [take(3) for _ in colors], [take(3) for _ in colors]
    in_q, in_n, in_m = [take(3) for _ in colors], [take(3) for _ in colors], [take(3) for _ in colors]
    stats_in, send_sem, recv_sem = take(3)
    spots = {}

    def remote(source, target, key, peer):
        at = spots.setdefault(key, len(spots))
        return pltpu.make_async_remote_copy(
            src_ref=source,
            dst_ref=target,
            send_sem=send_sem.at[at],
            recv_sem=recv_sem.at[at],
            device_id=(peer,),
            device_id_type=MESH,
        )

    def mine(axis):
        size, stride = axis
        return (me // stride) % size

    stats_copy = remote(stats_ref, stats_in, "stats", partner)
    stats_copy.start()

    nodes, width = grad_ref.shape
    own_neg = ids_ref.shape[0]
    slot, ids = id_column(ids_ref)
    node = lax.broadcasted_iota(jnp.int32, (nodes, 1), 0)
    named = jnp.zeros((nodes, 1), jnp.bool_)
    for j in range(own_neg):
        named = named | (node == ids_ref[j])
    pre = jnp.where(named, 0.0, grad_ref[...]).astype(BF16)
    lanes = lax.broadcasted_iota(jnp.int32, (own_neg, nodes), 1)
    pick = jnp.where(ids == lanes, 1.0, 0.0)
    local = jnp.dot(pick, grad_ref[...], preferred_element_type=F32, precision=lax.Precision.HIGHEST)
    rows = full[0].shape[5]
    pairs = []
    wide = 2 * LANES
    for half in range(0, count, 2):
        block = slice(half * LANES, half * LANES + wide)
        for color in (half, half + 1):
            axes = colors[color]
            for c in range(2):
                for spot in spots_of(axes):
                    at = device_of(axes, c, spot) * own_neg
                    full_neg[color][(c, *spot)] = neg_ref[at : at + own_neg, color * LANES : (color + 1) * LANES]
        for term in range(terms):
            left = own_ref[...] if term == 0 else means_ref[term - 1]
            product = tn(left, pre[:, block])
            for color in (half, half + 1):
                axes = colors[color]
                part = product[:, (color - half) * LANES : (color - half + 1) * LANES]
                for c in range(2):
                    for spot in spots_of(axes):
                        at = device_of(axes, c, spot) * rows
                        full[color][(c, *spot, term)] = part[at : at + rows]
        for color in (half, half + 1):
            pairs.append([
                remote(full[color].at[1 - core], paired[color], ("pair", color), partner),
                remote(full_neg[color].at[1 - core], paired_neg[color], ("pair_neg", color), partner),
            ])
            for copy in pairs[-1]:
                copy.start()

    def scatter(color, phase, stats):
        axis = colors[color][phase]
        size, stride = axis
        at = mine(axis)
        copies = []
        for delta in range(1, size):
            other = (at + delta) % size
            peer = me + (other - at) * stride
            block, neg = sums[color][phase][other], sums_neg[color][phase][other]
            scale, neg_scale = lane_scale(block), lane_scale(neg)
            spot = delta - 1
            out_q[color][phase][spot] = quantize(block, scale)
            out_n[color][phase][spot] = quantize(neg, neg_scale)
            out_m[color][phase][spot, 0:1] = scale
            out_m[color][phase][spot, 1:2] = neg_scale
            out_m[color][phase][spot, 2:4] = stats
            key = ("scatter", color, phase, delta)
            copies += [
                remote(out_q[color][phase].at[spot], in_q[color][phase].at[spot], (*key, 0), peer),
                remote(out_n[color][phase].at[spot], in_n[color][phase].at[spot], (*key, 1), peer),
                remote(out_m[color][phase].at[spot], in_m[color][phase].at[at], (*key, 2), peer),
            ]
        for copy in copies:
            copy.start()
        return copies

    def gather(color, phase):
        axes = colors[color]
        at = [mine(axis) for axis in axes]
        index = (core, *at[: phase + 1])
        copies = []
        if phase < 0:
            for kind, ref in enumerate((words[color], scales[color], rows_out[color])):
                copies.append(remote(ref.at[core], ref.at[core], ("gather", color, phase, 0, kind), partner))
        else:
            size, stride = axes[phase]
            for delta in range(1, size):
                peer = me + ((at[phase] + delta) % size - at[phase]) * stride
                for kind, ref in enumerate((words[color], scales[color], rows_out[color])):
                    copies.append(remote(ref.at[index], ref.at[index], ("gather", color, phase, delta, kind), peer))
        for copy in copies:
            copy.start()
        return copies

    stats_copy.wait()
    stats = [None] * count
    stats[0] = stats_ref[2:4] + stats_in[2:4]
    for color in range(1, count):
        stats[color] = stats[0]
    flying = []
    for color in range(count):
        for copy in pairs[color]:
            copy.wait()
        sums[color][0][...] = full[color][core] + paired[color][...]
        sums_neg[color][0][...] = full_neg[color][core] + paired_neg[color][...]
        flying.append(scatter(color, 0, stats[color]))
    lefts_wait()
    lefts_copy = remote(lefts_ref, lefts_out.at[core], "lefts", partner)
    lefts_copy.start()
    lefts_out[core] = lefts_ref[...]
    for phase in range(3):
        for color in range(count):
            axis = colors[color][phase]
            size = axis[0]
            at = mine(axis)
            for copy in flying[color]:
                copy.wait()
            total = sums[color][phase][at]
            total_neg = sums_neg[color][phase][at]
            for delta in range(1, size):
                meta = in_m[color][phase][(at + size - delta) % size]
                total = total + in_q[color][phase][delta - 1].astype(jnp.int32).astype(F32) * meta[0:1]
                total_neg = total_neg + in_n[color][phase][delta - 1].astype(jnp.int32).astype(F32) * meta[1:2]
            in_m[color][phase][at, 2:4] = stats[color]
            stats[color] = in_m[color][phase][0, 2:4]
            for position in range(1, size):
                stats[color] = stats[color] + in_m[color][phase][position, 2:4]
            if phase < 2:
                sums[color][phase + 1][...] = total
                sums_neg[color][phase + 1][...] = total_neg
                flying[color] = scatter(color, phase + 1, stats[color])
            else:
                index = (core, *(mine(a) for a in colors[color]))
                scale = lane_scale(total)
                words[color][index] = quantize(total, scale)
                scales[color][index] = scale
                gathered = local[:, color * LANES : (color + 1) * LANES]
                for j in range(own_neg):
                    gathered = gathered + jnp.where(ids == ids_ref[j], total_neg[j : j + 1], 0.0)
                rows_out[color][index] = gathered.astype(BF16)
                flying[color] = gather(color, 2)
    total_ref[0:2] = stats[0]
    again = jnp.zeros_like(ids)
    for j in range(own_neg):
        again = again + jnp.where((ids == ids_ref[j]) & (slot > j), 1, 0)
    pick = one_hot((ids == lanes) & (again == 0))
    for color in range(count):
        block = slice(color * LANES, (color + 1) * LANES)
        patch = tn(pick, rows_out[color][(core, *(mine(a) for a in colors[color]))])
        pre_ref[:, block] = jnp.where(named, patch, pre_ref[:, block].astype(F32)).astype(BF16)
    for phase in (1, 0, -1):
        for color in range(count):
            for copy in flying[color]:
                copy.wait()
            flying[color] = gather(color, phase)
    for color in range(count):
        for copy in flying[color]:
            copy.wait()
    lefts_copy.wait()


def finish_kernel(colors, pre_ref, lefts_ref, total_ref, *refs):
    count = len(colors)
    words, scales, rows_in = refs[:count], refs[count : 2 * count], refs[2 * count : 3 * count]
    out_ref, loss_ref, pre_out, joint = refs[3 * count :]
    term = pl.program_id(0)
    chips, own_neg = lefts_ref.shape[1], lefts_ref.shape[3]
    edges = total_ref[1:2]
    inverse = 1.0 / edges

    @pl.when(term == 0)
    def _():
        loss_ref[...] = total_ref[0:1] / edges
        for color, axes in enumerate(colors):
            for c in range(2):
                for spot in spots_of(axes):
                    at = (c * chips + device_of(axes, 0, spot) // 2) * own_neg
                    joint[at : at + own_neg, color * LANES : (color + 1) * LANES] = rows_in[color][(c, *spot)]
        pre_out[...] = pre_ref[...]

    lefts = lefts_ref[:, :, term].reshape(2 * chips * own_neg, lefts_ref.shape[4])
    extra = tn(lefts, joint[...])
    rows = words[0].shape[5]
    for color, axes in enumerate(colors):
        block = slice(color * LANES, (color + 1) * LANES)
        for c in range(2):
            for spot in spots_of(axes):
                at = device_of(axes, c, spot) * rows
                value = words[color][(c, *spot, term)].astype(jnp.int32).astype(F32) * scales[color][(c, *spot)]
                out_ref[0, at : at + rows, block] = (value + extra[at : at + rows, block]) * inverse


def call(kernel, out_shape, in_specs, collective=None, **kwargs):
    extra = {} if collective is None else {"collective_id": collective, "has_side_effects": True}
    many = isinstance(out_shape, (list, tuple))
    return pl.pallas_call(
        kernel,
        out_shape=out_shape,
        in_specs=in_specs,
        out_specs=whole(len(out_shape)) if many else whole(1)[0],
        compiler_params=pltpu.CompilerParams(vmem_limit_bytes=VMEM_LIMIT, **extra),
        **kwargs,
    )


def shape(dims, kind):
    return jax.ShapeDtypeStruct(dims, kind)


def on_device(parts, features, weights, halo_send, nbr_index, tile_count, edge_ends, neg_ids):
    nodes, width = features.shape
    relations, fan = nbr_index.shape[1:]
    per_peer = halo_send.shape[2]
    slots = nodes + parts * per_peer
    own_neg = neg_ids.shape[0]
    hbm = pl.BlockSpec(memory_space=pltpu.HBM)
    chips = parts // 2
    terms = relations + 1
    edges = edge_ends.shape[0] * edge_ends.shape[2]
    orders = layout(parts)
    colors = [orders[color % 2] for color in range(width // LANES)]
    block, neg_block = (terms, width // parts, LANES), (own_neg, LANES)
    outs, scratch = [], []
    for tail, kind in ((block, jnp.int16), ((1, LANES), F32), (neg_block, BF16)):
        outs += [shape((2, *sizes(axes), *tail), kind) for axes in colors]
    outs += [
        shape((2, chips, terms, own_neg, width), BF16),
        shape((2, LANES), F32),
        shape((nodes, width), BF16),
    ]
    scratch += [
        pltpu.SMEM(neg_ids.shape, jnp.int32),
        pltpu.VMEM((nodes, width), BF16),
        pltpu.VMEM((relations, nodes, width), BF16),
        pltpu.VMEM((nodes, width), F32),
        pltpu.VMEM((parts * own_neg, width), F32),
        pltpu.VMEM((8, LANES), F32),
        pltpu.VMEM(weights.shape, BF16),
        pltpu.VMEM((relations * fan, nodes), jnp.int32),
        pltpu.VMEM((nodes, relations * fan), jnp.int32),
        pltpu.VMEM((per_peer, parts), jnp.int32),
        pltpu.VMEM(edge_ends.shape, jnp.int32),
        pltpu.VMEM((relations, nodes, slots), BF16),
        pltpu.VMEM((relations, nodes, width), F32),
        pltpu.VMEM((nodes, width), F32),
        pltpu.VMEM((nodes, edges), BF16),
        pltpu.VMEM((nodes, edges), BF16),
        pltpu.VMEM((nodes, nodes), F32),
        pltpu.VMEM((nodes, width), BF16),
        pltpu.VMEM((parts, per_peer, width), BF16),
        pltpu.VMEM((parts, per_peer, width), BF16),
        pltpu.VMEM((own_neg, width), BF16),
        pltpu.VMEM((parts, own_neg, width), BF16),
        pltpu.VMEM((terms, own_neg, width), BF16),
        pltpu.VMEM((chips, terms, own_neg, width), BF16),
        pltpu.SemaphoreType.DMA((6,)),
        pltpu.SemaphoreType.DMA((3, parts)),
        pltpu.SemaphoreType.DMA((3, parts)),
    ]
    for lead in ((2,), ()):
        for tail in (block, neg_block):
            scratch += [pltpu.VMEM((*lead, *sizes(axes), *tail), F32) for axes in colors]
    for tail in (block, neg_block):
        for axes in colors:
            scratch += [pltpu.VMEM((*sizes(axes)[phase:], *tail), F32) for phase in range(3)]
    for inbound in (False, True):
        for tail in (block, neg_block):
            for axes in colors:
                dims = sizes(axes)
                scratch += [pltpu.VMEM((dims[phase] - 1, *dims[phase + 1 :], *tail), jnp.int16) for phase in range(3)]
        for axes in colors:
            scratch += [pltpu.VMEM((size if inbound else size - 1, 8, LANES), F32) for size in sizes(axes)]
    scratch.append(pltpu.VMEM((8, LANES), F32))
    copies = 2 + sum(5 + 6 * sum(size - 1 for size in sizes(axes)) for axes in colors)
    scratch += [pltpu.SemaphoreType.DMA((copies,)), pltpu.SemaphoreType.DMA((copies,))]
    reduced = call(
        functools.partial(step_kernel, colors, fan),
        tuple(outs),
        [hbm] * 6 + [pl.BlockSpec(memory_space=pltpu.SMEM)],
        collective=2,
        scratch_shapes=scratch,
    )(
        *(
            pltpu.with_memory_space_constraint(x, pltpu.HBM)
            for x in (
                halo_send[0].T,
                features,
                nbr_index.transpose(1, 2, 0).reshape(relations * fan, nodes),
                weights,
                edge_ends,
                neg_ids,
            )
        ),
        tile_count,
    )
    gathered, (lefts, total, pre) = reduced[:-3], reduced[-3:]
    weight_grad, loss, pre_grad = pl.pallas_call(
        functools.partial(finish_kernel, colors),
        grid=(terms,),
        out_shape=(shape((terms, width, width), F32), shape((1, LANES), F32), shape((nodes, width), BF16)),
        in_specs=whole(3 + len(gathered)),
        out_specs=(
            pl.BlockSpec((1, width, width), lambda term: (term, 0, 0)),
            pl.BlockSpec((1, LANES), lambda term: (0, 0)),
            pl.BlockSpec((nodes, width), lambda term: (0, 0)),
        ),
        scratch_shapes=[pltpu.VMEM((parts * own_neg, width), BF16)],
        compiler_params=pltpu.CompilerParams(vmem_limit_bytes=VMEM_LIMIT),
    )(pre, lefts, total, *gathered)
    return (weight_grad, loss[0, 0], pre_grad)


def solution(mesh):
    placed = (
        P("dom", None),
        P(),
        P("dom", None, None),
        P("dom", None, None),
        P("dom"),
        P("dom", None, None),
        P("dom"),
    )
    return jax.shard_map(
        functools.partial(on_device, mesh.shape["dom"]),
        mesh=mesh,
        in_specs=placed,
        out_specs=(P(), P(), P("dom", None)),
        check_vma=False,
    )
```
